32 devices in a mesh: dp: 2 (over x), tp: 16 (over y, z, core).
Axes of the slice: x: 2, y: 2, z: 4, core: 2. Of those that a mesh axis runs over, the one named last changes fastest.
Arguments:
- x: bfloat16 [4096, 8192], P('dp'), parts along dimension 0
- gain: bfloat16 [8192], replicated
- wq: bfloat16 [8192, 8192], P(None, 'tp')
- wk: bfloat16 [8192, 8192], P(None, 'tp')
- wv: bfloat16 [8192, 8192], P(None, 'tp')
- wo: bfloat16 [8192, 8192], P('tp')
Outputs:
- output: bfloat16 [4096, 8192], P('dp'), parts along dimension 0
There are 2 independent parts. The reference program is written for one: setup_inputs(seed, part) draws one part's arguments, and reference() takes and returns one part's arrays. A program takes and returns all parts, laid end to end along the dimension named above; an argument that names none is the same for every part.
All inputs are finite; a program needn't handle non-finite values.
Results may differ from the reference program's by a relative error of at most 0.012.
Values are sent between devices in bfloat16 or wider.
A program may use at most 2 GiB of HBM per device.

```python
import jax
import jax.numpy as jnp
from jax import lax

ROWS = 2048
D = 8192
HEADS = 64
KV_HEADS = 64
HEAD = 128
THETA = 10000


def setup_inputs(seed: int = 0, part: int = 0) -> dict:
    kx, kn, kq, kk, kv, ko = jax.random.split(jax.random.key(seed), 6)

    def weights(key, rows, columns):
        return jax.random.normal(key, (rows, columns), jnp.float32) * rows**-0.5

    drawn = {
        "x": jax.random.normal(jax.random.fold_in(kx, part), (ROWS, D), jnp.float32),
        "gain": 1 + 0.1 * jax.random.normal(kn, (D,), jnp.float32),
        "wq": 2 * weights(kq, D, HEADS * HEAD),
        "wk": 2 * weights(kk, D, KV_HEADS * HEAD),
        "wv": 4 * weights(kv, D, KV_HEADS * HEAD),
        "wo": weights(ko, HEADS * HEAD, D),
    }
    return {k: v.astype(jnp.bfloat16) for k, v in drawn.items()}


def normed(x, gain):
    wide = x.astype(jnp.float32)
    scale = lax.rsqrt(jnp.mean(wide * wide, -1, keepdims=True) + 1e-6)
    return (wide * scale * gain.astype(jnp.float32)).astype(jnp.bfloat16)


def turned(t, place, theta):
    half = t.shape[-1] // 2
    angle = place.astype(jnp.float32)[:, None] * theta ** (-jnp.arange(half, dtype=jnp.float32) / half)
    cos, sin = jnp.cos(angle)[:, None], jnp.sin(angle)[:, None]
    a, b = t[..., :half].astype(jnp.float32), t[..., half:].astype(jnp.float32)
    return jnp.concatenate([a * cos - b * sin, b * cos + a * sin], -1).astype(jnp.bfloat16)


def matmul(a, w):
    return jnp.dot(a, w, preferred_element_type=jnp.float32).astype(jnp.bfloat16)


def einsum(form, a, b):
    return jnp.einsum(form, a.astype(jnp.float32), b.astype(jnp.float32))


def attention(q, k, v):
    scores = einsum("tgsd,ugd->gstu", q, k) * q.shape[-1] ** -0.5
    token = jnp.arange(q.shape[0])
    scores = jnp.where(token[:, None] >= token, scores, -jnp.inf)
    weights = jax.nn.softmax(scores, -1).astype(jnp.bfloat16)
    return einsum("gstu,ugd->tgsd", weights, v).astype(jnp.bfloat16)


def reference(x, gain, wq, wk, wv, wo):
    a, place = normed(x, gain), jnp.arange(ROWS)
    q = turned(matmul(a, wq).reshape(ROWS, HEADS, HEAD), place, THETA).reshape(ROWS, KV_HEADS, -1, HEAD)
    k = turned(matmul(a, wk).reshape(ROWS, KV_HEADS, HEAD), place, THETA)
    v = matmul(a, wv).reshape(ROWS, KV_HEADS, HEAD)
    seen = attention(q, k, v).reshape(ROWS, HEADS * HEAD)
    return (x.astype(jnp.float32) + jnp.dot(seen, wo, preferred_element_type=jnp.float32)).astype(jnp.bfloat16)
```

```python
import functools

import jax
import jax.numpy as jnp
from jax import lax
from jax.experimental import pallas as pl
from jax.experimental.pallas import tpu as pltpu
from jax.sharding import PartitionSpec as P

HEAD = 128
THETA = 10000
NEG = -1e30
HIDDEN = 2 * NEG
LOG2E = 1.4426950408889634
MESH = pl.DeviceIdType.MESH
VMEM = 56 * 2**20
STRIP = 512


def _dot(a, b, ca, cb):
    return lax.dot_general(a, b, (((ca,), (cb,)), ((), ())), preferred_element_type=jnp.float32)


def _attend(q_ref, k_ref, v_ref, o_ref, top_s, mix_s, gap_s, *, scale, bq, bk):
    heads, _, d = q_ref.shape
    iq = pl.program_id(0)
    low = k_ref.dtype
    e = scale * LOG2E
    wide = min(bq, STRIP)
    pieces = [(i, at) for i in range(heads) for at in range(0, bq, wide)]
    gap_s[...] = lax.broadcasted_iota(jnp.int32, (bk, bq), 1) - lax.broadcasted_iota(jnp.int32, (bk, bq), 0)
    top_s[...] = jnp.full(top_s.shape, NEG, jnp.float32)
    mix_s[...] = jnp.zeros(mix_s.shape, jnp.float32)
    ones = jnp.ones((8, bk), low)

    def block(j, masked):
        here = pl.ds(j * bk, bk)
        scores = [_dot(k_ref[i, here, :], q_ref[i, at : at + wide, :], 1, 1) for i, at in pieces]
        ok = gap_s[...] >= j * bk - iq * bq if masked else None
        weights, keeps = [], []
        for (i, at), s in zip(pieces, scores):
            if masked:
                s = jnp.where(ok[:, at : at + wide], s, HIDDEN)
            old = top_s[i : i + 1, at : at + wide]
            top = jnp.maximum(old, s.max(axis=0, keepdims=True))
            top_s[i : i + 1, at : at + wide] = top
            weights.append(jnp.exp2((s - top) * e).astype(low))
            keeps.append(jnp.exp2((old - top) * e))
        for (i, at), p, keep in zip(pieces, weights, keeps):
            values = jnp.concatenate([v_ref[i, here, :].T, ones], axis=0)
            mix_s[i, :, at : at + wide] = mix_s[i, :, at : at + wide] * keep + _dot(values, p, 1, 0)

    whole = lax.div(iq * bq + 1, bk)
    lax.fori_loop(0, whole, lambda j, _: block(j, False), None)
    lax.fori_loop(whole, lax.div(iq * bq + bq + bk - 1, bk), lambda j, _: block(j, True), None)
    for i in range(heads):
        o_ref[:, i * d : (i + 1) * d] = (mix_s[i, :d, :] * (1 / mix_s[i, d : d + 1, :])).T.astype(o_ref.dtype)


def attend(q, k, v, bq, bk):
    heads, tokens, d = q.shape
    keys = pl.BlockSpec((heads, tokens, d), lambda iq: (0, 0, 0))
    return pl.pallas_call(
        functools.partial(_attend, scale=d**-0.5, bq=bq, bk=bk),
        grid=(tokens // bq,),
        in_specs=[pl.BlockSpec((heads, bq, d), lambda iq: (0, iq, 0)), keys, keys],
        out_specs=pl.BlockSpec((bq, heads * d), lambda iq: (iq, 0)),
        out_shape=jax.ShapeDtypeStruct((tokens, heads * d), q.dtype),
        scratch_shapes=[pltpu.VMEM((heads, bq), jnp.float32), pltpu.VMEM((heads, d + 8, bq), jnp.float32), pltpu.VMEM((bk, bq), jnp.int32)],
        compiler_params=pltpu.CompilerParams(dimension_semantics=("arbitrary",), vmem_limit_bytes=VMEM),
        cost_estimate=pl.CostEstimate(flops=4 * heads * tokens * tokens * d, transcendentals=heads * tokens * tokens,
                                      bytes_accessed=8 * heads * tokens * d),
    )(q, k, v)


def _project(x_ref, gain_ref, cos_ref, sin_ref, wq_ref, wk_ref, wv_ref, q_ref, k_ref, v_ref, a_s, wq_s, wk_s, wv_s, sem):
    pairs = [(wq_ref, wq_s), (wk_ref, wk_s), (wv_ref, wv_s)]
    copies = [pltpu.make_async_copy(src, dst, sem.at[n]) for n, (src, dst) in enumerate(pairs)]
    first = pl.program_id(0) == 0

    @pl.when(first)
    def _():
        for copy in copies:
            copy.start()

    rows, width = a_s.shape
    step = 16

    def norm(n, _):
        at = pl.ds(n * step, step)
        wide = x_ref[at, :].astype(jnp.float32)
        scale = lax.rsqrt(jnp.mean(wide * wide, -1, keepdims=True) + 1e-6)
        a_s[at, :] = (wide * scale * gain_ref[...].astype(jnp.float32)).astype(jnp.bfloat16)

    lax.fori_loop(0, rows // step, norm, None)
    for n, (w, out, turn) in enumerate(((wq_s, q_ref, True), (wk_s, k_ref, True), (wv_s, v_ref, False))):
        @pl.when(first)
        def _(n=n):
            copies[n].wait()

        got = _dot(a_s[...], w[...], 1, 0).astype(jnp.bfloat16)
        for h in range(out.shape[0]):
            t = got[:, h * HEAD : (h + 1) * HEAD]
            if turn:
                t = t.astype(jnp.float32)
                t = (t * cos_ref[...] + pltpu.roll(t, HEAD // 2, 1) * sin_ref[...]).astype(jnp.bfloat16)
            out[h] = t


def project(x, gain, wq, wk, wv, rows):
    tokens, width = x.shape
    part = wq.shape[1]
    heads = part // HEAD
    half = HEAD // 2
    angle = jnp.arange(tokens).astype(jnp.float32)[:, None] * THETA ** (-jnp.arange(half, dtype=jnp.float32) / half)
    cos, sin = jnp.cos(angle), jnp.sin(angle)
    cos, sin = jnp.concatenate([cos, cos], -1), jnp.concatenate([-sin, sin], -1)
    table = pl.BlockSpec((rows, HEAD), lambda i: (i, 0))
    whole = pl.BlockSpec(memory_space=pl.ANY)
    out = pl.BlockSpec((heads, rows, HEAD), lambda i: (0, i, 0))
    weights = pltpu.VMEM((width, part), jnp.bfloat16)
    return pl.pallas_call(
        _project,
        grid=(tokens // rows,),
        in_specs=[pl.BlockSpec((rows, width), lambda i: (i, 0)), pl.BlockSpec((1, width), lambda i: (0, 0)), table, table, whole, whole, whole],
        out_specs=[out] * 3,
        out_shape=[jax.ShapeDtypeStruct((heads, tokens, HEAD), jnp.bfloat16)] * 3,
        scratch_shapes=[pltpu.VMEM((rows, width), jnp.bfloat16), weights, weights, weights, pltpu.SemaphoreType.DMA((3,))],
        compiler_params=pltpu.CompilerParams(dimension_semantics=("arbitrary",), vmem_limit_bytes=VMEM),
        cost_estimate=pl.CostEstimate(flops=6 * tokens * width * part, transcendentals=0, bytes_accessed=2 * width * (tokens + 3 * part)),
    )(x, gain[None], cos, sin, wq, wk, wv)


def finish(seen, wo, across, x, *, rows, keep, lags, ahead, tile):
    tokens, depth = seen.shape
    wide = x.shape[1]
    quarter, half = wide // 4, wide // 8
    count = tokens // rows
    d2, d3, d4, d5, d6 = lags

    def kernel(seen_ref, wo_ref, across_ref, x_ref, out_ref, seen4, wo4, big, sums, xs, acc_s,
               seen_sem, red_sem, own_sem, nbr_y, nbr_z, par_sem, dia_sem, wo_sem, local_sem, x_sem, send_sem):
        me = lax.axis_index("tp")
        y, z, c = me // 8, (me // 2) % 4, me % 2
        s = z // 2
        o = 1 - s
        inner = (z == 1) | (z == 2)
        at = lambda y, z, c: (y * 4 + z) * 2 + c
        partner, over = at(y, z, 1 - c), at(1 - y, z, c)
        peer = at(y, 3 - z, c)
        side = at(y, jnp.where(inner, 3 * s, 1 + s), c)
        block = y * 2 + c
        nblock = (1 - y) * 2 + c

        barrier = pltpu.get_barrier_semaphore()
        for who in (partner, over, side):
            pl.semaphore_signal(barrier, inc=1, device_id={"tp": who}, device_id_type=MESH)

        @pl.when(inner)
        def _():
            pl.semaphore_signal(barrier, inc=1, device_id={"tp": peer}, device_id_type=MESH)
            pl.semaphore_wait(barrier, 4)

        @pl.when(jnp.logical_not(inner))
        def _():
            pl.semaphore_wait(barrier, 3)

        def there(src, dst, kind, recv, who):
            pltpu.make_async_remote_copy(src_ref=src, dst_ref=dst, send_sem=send_sem.at[kind], recv_sem=recv, device_id={"tp": who},
                                         device_id_type=MESH).start()

        def arrived(dst, sem):
            pltpu.make_async_copy(dst, dst, sem).wait()

        def span(i):
            return pl.ds(pl.multiple_of(i * rows, rows), rows)

        def cols(q, h, a, b):
            return pl.ds(pl.multiple_of(q * quarter + h * half + a, 128), b - a)

        def blk(b):
            return pl.ds(pl.multiple_of(b * depth, 128), depth)

        mine = pltpu.make_async_copy(seen_ref, seen4.at[:, blk(block)], local_sem.at[0])
        mine.start()

        def wo_part(src, side_block, h):
            return src.at[:, pl.ds(pl.multiple_of(side_block * quarter + h * half, 128), half)]

        def rows_of(b):
            return pl.ds(pl.multiple_of(b * depth, 128), depth)

        def send_seen(i):
            there(seen_ref.at[span(i), :], seen4.at[span(i), blk(block)], 0, seen_sem.at[1, i], over)
            there(seen_ref.at[span(i), :], seen4.at[span(i), blk(block)], 1, seen_sem.at[0, i], partner)

        for i in range(min(ahead, count)):
            send_seen(i)
        for h in range(2):
            there(wo_part(wo_ref, y * 2 + 1 - c, h), wo4.at[h, rows_of(block), :], 2, wo_sem.at[0, h], partner)
            there(wo_part(across_ref, 1 - c, h), wo4.at[h, rows_of(nblock), :], 3, wo_sem.at[1, h], partner)
            pltpu.make_async_copy(wo_part(wo_ref, y * 2 + c, h), wo4.at[h, rows_of(block), :], wo_sem.at[2, h]).start()
            pltpu.make_async_copy(wo_part(across_ref, c, h), wo4.at[h, rows_of(nblock), :], wo_sem.at[3, h]).start()

        pblock, dblock = y * 2 + 1 - c, (1 - y) * 2 + 1 - c

        def wo_wait():
            for h in range(2):
                arrived(wo4.at[h, rows_of(pblock), :], wo_sem.at[0, h])
                arrived(wo4.at[h, rows_of(dblock), :], wo_sem.at[1, h])
                arrived(wo4.at[h, rows_of(block), :], wo_sem.at[2, h])
                arrived(wo4.at[h, rows_of(nblock), :], wo_sem.at[3, h])

        mine.wait()

        def term(i, h, n):
            return jnp.dot(seen4[span(i), :], wo4[h, :, pl.ds(pl.multiple_of(n * tile, tile), tile)], preferred_element_type=jnp.float32)

        def tiles(body):
            def step(n, _):
                body(n, pl.ds(pl.multiple_of(n * tile, tile), tile))
            lax.fori_loop(0, half // tile, step, None)

        def seen_ready(i):
            arrived(seen4.at[span(i), blk(pblock)], seen_sem.at[0, i])
            arrived(seen4.at[span(i), blk(dblock)], seen_sem.at[2, i])

        def out_at(i, q, h, a=0, b=half):
            return out_ref.at[span(i), cols(q, h, a, b)]

        def x_copy(i):
            return pltpu.make_async_copy(x_ref.at[span(i), cols(block, s, 0, half)], xs.at[lax.rem(i, 2)], x_sem.at[lax.rem(i, 2)])

        def tick(t, _):
            on = lambda lag: (t >= lag) & (t - lag < count)

            if ahead < count:
                @pl.when(t + ahead < count)
                def _():
                    send_seen(t + ahead)

            @pl.when(t < count)
            def _():
                arrived(seen4.at[span(t), blk(nblock)], seen_sem.at[1, t])
                there(seen4.at[span(t), blk(nblock)], seen4.at[span(t), blk(nblock)], 4, seen_sem.at[2, t], partner)

            @pl.when(t == min(d2, d3))
            def _():
                wo_wait()

            @pl.when(jnp.logical_not(inner))
            def _():
                @pl.when(on(d2))
                def _():
                    i = t - d2
                    seen_ready(i)
                    for k, h in enumerate((o, s)):
                        def put(n, at, h=h):
                            big[h, span(i), at] = term(i, h, n).astype(jnp.bfloat16)
                        tiles(put)
                        there(big.at[h, span(i), :], big.at[h, span(i), :], 5, red_sem.at[k, i], side)

                @pl.when(on(d6))
                def _():
                    i = t - d6
                    for h in (s, o):
                        arrived(out_at(i, block, h), own_sem.at[h, i])
                        if keep:
                            there(out_at(i, block, h, 0, keep), out_at(i, block, h, 0, keep), 6, nbr_y.at[h, i], over)
                        there(out_at(i, block, h), out_at(i, block, h), 7, par_sem.at[h, i], partner)

                @pl.when(on(d6 + 1))
                def _():
                    i = t - d6 - 1
                    for h in (s, o):
                        if keep < half:
                            arrived(out_at(i, nblock, h, keep, half), nbr_z.at[h, i])
                        if keep:
                            arrived(out_at(i, nblock, h, 0, keep), nbr_y.at[h, i])
                        there(out_at(i, nblock, h), out_at(i, nblock, h), 8, dia_sem.at[h, i], partner)

            @pl.when(inner)
            def _():
                @pl.when(on(d3))
                def _():
                    i = t - d3
                    seen_ready(i)
                    arrived(big.at[o, span(i), :], red_sem.at[0, i])

                    def add(n, at):
                        sums[o, span(i), at] = (term(i, o, n) + big[o, span(i), at].astype(jnp.float32)).astype(jnp.bfloat16)
                    tiles(add)
                    there(sums.at[o, span(i), :], sums.at[o, span(i), :], 9, red_sem.at[2, i], peer)
                    x_copy(i).start()

                @pl.when(on(d4))
                def _():
                    i = t - d4
                    slot = lax.rem(i, 2)
                    x_copy(i).wait()
                    arrived(big.at[s, span(i), :], red_sem.at[1, i])

                    def before(n, at):
                        acc_s[:, at] = term(i, s, n) + big[s, span(i), at].astype(jnp.float32) + xs[slot, :, at].astype(jnp.float32)
                    tiles(before)
                    arrived(sums.at[s, span(i), :], red_sem.at[2, i])

                    def add(n, at):
                        big[s, span(i), at] = (acc_s[:, at] + sums[s, span(i), at].astype(jnp.float32)).astype(jnp.bfloat16)
                    tiles(add)
                    done = big.at[s, span(i), :]
                    there(done, out_at(i, block, s), 10, own_sem.at[s, i], peer)
                    there(done, out_at(i, block, s), 11, own_sem.at[s, i], side)
                    if keep < half:
                        there(big.at[s, span(i), pl.ds(keep, half - keep)], out_at(i, block, s, keep, half), 12, nbr_z.at[s, i], over)
                    if keep:
                        there(big.at[s, span(i), pl.ds(0, keep)], out_at(i, block, s, 0, keep), 6, nbr_y.at[s, i], over)
                    there(done, out_at(i, block, s), 7, par_sem.at[s, i], partner)
                    pltpu.make_async_copy(done, out_at(i, block, s), local_sem.at[1]).start()

                @pl.when(on(d5))
                def _():
                    i = t - d5
                    arrived(out_at(i, block, o), own_sem.at[o, i])
                    there(out_at(i, block, o), out_at(i, block, o), 13, own_sem.at[o, i], side)
                    if keep:
                        there(out_at(i, block, o, 0, keep), out_at(i, block, o, 0, keep), 6, nbr_y.at[o, i], over)
                    there(out_at(i, block, o), out_at(i, block, o), 7, par_sem.at[o, i], partner)
                    if keep < half:
                        far = out_at(i, nblock, s, keep, half)
                        arrived(far, nbr_z.at[s, i])
                        there(far, far, 14, nbr_z.at[s, i], peer)
                        there(far, far, 15, nbr_z.at[s, i], side)
                    if keep:
                        arrived(out_at(i, nblock, s, 0, keep), nbr_y.at[s, i])
                    there(out_at(i, nblock, s), out_at(i, nblock, s), 8, dia_sem.at[s, i], partner)

                @pl.when(on(d5 + 1))
                def _():
                    i = t - d5 - 1
                    if keep < half:
                        far = out_at(i, nblock, o, keep, half)
                        arrived(far, nbr_z.at[o, i])
                        there(far, far, 16, nbr_z.at[o, i], side)
                    if keep:
                        arrived(out_at(i, nblock, o, 0, keep), nbr_y.at[o, i])
                    there(out_at(i, nblock, o), out_at(i, nblock, o), 8, dia_sem.at[o, i], partner)

        lax.fori_loop(0, count + max(d5, d6) + 1, tick, None)

        def last(i, _):
            for h in range(2):
                arrived(out_at(i, pblock, h), par_sem.at[h, i])
                arrived(out_at(i, dblock, h), dia_sem.at[h, i])
        lax.fori_loop(0, count, last, None)

        def sent(kind, ref):
            pltpu.make_async_copy(ref, ref, send_sem.at[kind]).wait()

        sent(0, seen_ref)
        sent(1, seen_ref)
        sent(2, wo4.at[:, pl.ds(0, depth), :])
        sent(3, wo4.at[:, pl.ds(0, depth), :])
        sent(4, seen_ref)
        full = lambda n, a, b: out_ref.at[:, pl.ds(0, n * (b - a))]
        if keep:
            sent(6, full(2, 0, keep))
        sent(7, full(2, 0, half))
        sent(8, full(2, 0, half))

        @pl.when(jnp.logical_not(inner))
        def _():
            sent(5, big)

        @pl.when(inner)
        def _():
            sent(9, full(1, 0, half))
            sent(10, full(1, 0, half))
            sent(11, full(1, 0, half))
            sent(13, full(1, 0, half))
            if keep < half:
                for kind in (12, 14, 15, 16):
                    sent(kind, full(1, keep, half))
            pltpu.make_async_copy(big.at[0], big.at[0], local_sem.at[1]).wait()

    any_ = pl.BlockSpec(memory_space=pl.ANY)
    dma = pltpu.SemaphoreType.DMA
    return pl.pallas_call(
        kernel,
        out_shape=jax.ShapeDtypeStruct((tokens, wide), jnp.bfloat16),
        in_specs=[any_] * 4,
        out_specs=any_,
        scratch_shapes=[
            pltpu.VMEM((tokens, 4 * depth), jnp.bfloat16),
            pltpu.VMEM((2, 4 * depth, half), jnp.bfloat16),
            pltpu.VMEM((2, tokens, half), jnp.bfloat16),
            pltpu.VMEM((2, tokens, half), jnp.bfloat16),
            pltpu.VMEM((2, rows, half), jnp.bfloat16),
            pltpu.VMEM((rows, half), jnp.float32),
            dma((3, count)), dma((3, count)), dma((2, count)), dma((2, count)), dma((2, count)), dma((2, count)), dma((2, count)),
            dma((4, 2)), dma((2,)), dma((2,)), dma((17,)),
        ],
        compiler_params=pltpu.CompilerParams(collective_id=0, has_side_effects=True, vmem_limit_bytes=56 * 2**20),
        cost_estimate=pl.CostEstimate(flops=2 * tokens * 4 * depth * quarter, transcendentals=0, bytes_accessed=4 * tokens * wide),
    )(seen, wo, across, x)


LAGS = (1, 1, 2, 3, 4)
AHEAD = 3
ROWS = 128
KEEP = 768


def solution(mesh):
    def step(x, gain, wq, wk, wv, wo):
        width = wo.shape[1]
        y = lax.axis_index("tp") // 8
        other = lax.dynamic_slice_in_dim(wo, (1 - y) * (width // 2), width // 2, 1)
        across = lax.ppermute(other, "tp", [(j, j ^ 8) for j in range(16)])
        q, k, v = project(x, gain, wq, wk, wv, 256)
        seen = attend(q, k, v, 1024, 512)
        return finish(seen, wo, across, x, rows=ROWS, keep=KEEP, lags=LAGS, ahead=AHEAD, tile=256)

    tokens, columns = P("dp", None), P(None, "tp")
    return jax.shard_map(
        step,
        mesh=mesh,
        in_specs=(tokens, P(None), columns, columns, columns, P("tp", None)),
        out_specs=tokens,
        check_vma=False,
    )
```

```python
import jax
import jax.numpy as jnp
import numpy as np
from jax import lax
from jax.experimental import pallas as pl
from jax.experimental.pallas import tpu as pltpu
from jax.sharding import PartitionSpec as P

HEAD = 128
THETA = 10000
NEG = -1e30
HIDDEN = 2 * NEG
LOG2E = 1.4426950408889634
MESH = pl.DeviceIdType.MESH
VMEM = 56 * 2**20


def _dot(a, b, ca, cb):
    return lax.dot_general(a, b, (((ca,), (cb,)), ((), ())), preferred_element_type=jnp.float32)


def attend_block(b, qkv_ref, o_ref, place, top_s, mix_s, gap_s, bq, bk):
    heads, d = qkv_ref.shape[0] // 3, qkv_ref.shape[2]
    low = qkv_ref.dtype
    e = d**-0.5 * LOG2E
    queries = pl.ds(pl.multiple_of(b * bq, bq), bq)
    top_s[...] = jnp.full(top_s.shape, NEG, jnp.float32)
    mix_s[...] = jnp.zeros(mix_s.shape, jnp.float32)
    ones = jnp.ones((8, bk), low)

    def block(j, masked):
        here = pl.ds(pl.multiple_of(j * bk, bk), bk)
        scores = [_dot(qkv_ref[heads + i, here, :], qkv_ref[i, queries, :], 1, 1) for i in range(heads)]
        ok = gap_s[...] >= j * bk - b * bq if masked else None
        weights, keeps = [], []
        for i, s in enumerate(scores):
            if masked:
                s = jnp.where(ok, s, HIDDEN)
            old = top_s[i : i + 1, :]
            top = jnp.maximum(old, s.max(axis=0, keepdims=True))
            top_s[i : i + 1, :] = top
            weights.append(jnp.exp2((s - top) * e).astype(low))
            keeps.append(jnp.exp2((old - top) * e))
        for i, (p, keep) in enumerate(zip(weights, keeps)):
            values = jnp.concatenate([qkv_ref[2 * heads + i, here, :].T, ones], axis=0)
            mix_s[i] = mix_s[i] * keep + _dot(values, p, 1, 0)

    whole = lax.div(b * bq + 1, bk)
    lax.fori_loop(0, whole, lambda j, _: block(j, False), None)
    lax.fori_loop(whole, lax.div(b * bq + bq + bk - 1, bk), lambda j, _: block(j, True), None)
    for i in range(heads):
        got = (mix_s[i, :d, :] * (1 / mix_s[i, d : d + 1, :])).T.astype(o_ref.dtype)
        o_ref[queries, pl.ds(pl.multiple_of((place * heads + i) * d, d), d)] = got


PIECES = 8


def _project(x_ref, gain_ref, table_ref, wq_ref, wk_ref, wv_ref, wo_ref, out_ref, across_ref, even_s, odd_s, w_s, w_sem, y_sem, x_sem, send_sem):
    i, last = pl.program_id(0), pl.num_programs(0) - 1
    me, dp = lax.axis_index("tp"), lax.axis_index("dp")
    y = me // 8
    over = lax.rem(me + 8, 16)
    rows, width = even_s.shape
    part = wq_ref.shape[1]
    tile = 2 * HEAD
    tiles = 3 * part // tile
    lot = -(-rows // tiles // 16) * 16
    copies = [pltpu.make_async_copy(src, w_s.at[:, pl.ds(n * part, part)], w_sem.at[n]) for n, src in enumerate((wq_ref, wk_ref, wv_ref))]
    depth, side = across_ref.shape
    few = depth // 2 // PIECES

    def piece(ref, d, n, at):
        return ref.at[pl.ds(pl.multiple_of(d * (depth // 2) + n * few, few), few), pl.ds(pl.multiple_of(at, 128), side)]

    @pl.when(i == 0)
    def _():
        for copy in copies:
            copy.start()
        barrier = pltpu.get_barrier_semaphore()
        pl.semaphore_signal(barrier, inc=1, device_id={"tp": over}, device_id_type=MESH)
        pl.semaphore_signal(barrier, inc=1, device_id={"dp": 1 - dp}, device_id_type=MESH)
        pl.semaphore_wait(barrier, 2)

        def send(n, _):
            pltpu.make_async_remote_copy(src_ref=piece(wo_ref, dp, n, (1 - y) * side), dst_ref=piece(across_ref, dp, n, 0), send_sem=send_sem.at[0],
                                         recv_sem=y_sem.at[n], device_id={"tp": over}, device_id_type=MESH).start()
        lax.fori_loop(0, PIECES, send, None)

    def arrived(ref, sem):
        pltpu.make_async_copy(ref, ref, sem).wait()

    def forward(n):
        ref = piece(across_ref, dp, n, 0)
        arrived(ref, y_sem.at[n])
        pltpu.make_async_remote_copy(src_ref=ref, dst_ref=ref, send_sem=send_sem.at[1], recv_sem=x_sem.at[n], device_id={"dp": 1 - dp},
                                     device_id_type=MESH).start()

    def norm(to, n):
        at = pl.multiple_of(jnp.minimum(n * lot, rows - lot), 16)
        for r in range(0, lot, 16):
            here = pl.ds(at + r, 16)
            total = jnp.zeros((16, HEAD), jnp.float32)
            for c in range(0, width, HEAD):
                wide = x_ref[here, c : c + HEAD].astype(jnp.float32)
                total += wide * wide
            scale = lax.rsqrt(total.sum(-1, keepdims=True) * (1 / width) + 1e-6)
            for c in range(0, width, HEAD):
                wide = x_ref[here, c : c + HEAD].astype(jnp.float32)
                to[here, c : c + HEAD] = (wide * scale * gain_ref[:, c : c + HEAD].astype(jnp.float32)).astype(jnp.bfloat16)

    def product(of, n):
        got = _dot(of[...], w_s[:, pl.ds(pl.multiple_of(n * tile, tile), tile)], 1, 0).astype(jnp.bfloat16)
        table = table_ref[...]
        swapped = pltpu.roll(table, HEAD // 2, 1)
        first = lax.broadcasted_iota(jnp.int32, table.shape, 1) < HEAD // 2
        turn = n < 2 * part // tile
        cos = jnp.where(turn, jnp.where(first, table, swapped), 1.0)
        sin = jnp.where(turn, jnp.where(first, -swapped, table), 0.0)
        for h in range(2):
            t = got[:, h * HEAD : (h + 1) * HEAD].astype(jnp.float32)
            out_ref[2 * n + h] = (t * cos + pltpu.roll(t, HEAD // 2, 1) * sin).astype(jnp.bfloat16)

    def both(of, to):
        def step(n, _):
            @pl.when((i == 1) & (lax.rem(n, part // tile) == 0))
            def _():
                arrived(w_s.at[:, pl.ds(0, part)], w_sem.at[lax.div(n, part // tile)])

            product(of, n)
            norm(to, n)
        lax.fori_loop(0, tiles, step, None)

    @pl.when(i == 0)
    def _():
        lax.fori_loop(0, tiles, lambda n, _: norm(even_s, n), None)

    @pl.when(i > 0)
    def _():
        def some(n, _):
            forward(n)
        lax.fori_loop(lax.div((i - 1) * PIECES, last), lax.div(i * PIECES, last), some, None)

    odd = lax.rem(i, 2) == 1

    @pl.when(odd)
    def _():
        both(even_s, odd_s)

    @pl.when((i > 0) & jnp.logical_not(odd))
    def _():
        both(odd_s, even_s)

    @pl.when(i == last)
    def _():
        def end(n, _):
            arrived(piece(across_ref, 1 - dp, n, 0), x_sem.at[n])
        lax.fori_loop(0, PIECES, end, None)
        half = across_ref.at[pl.ds(0, depth // 2), :]
        arrived(half, send_sem.at[0])
        arrived(half, send_sem.at[1])


def project(x, gain, wq, wk, wv, wo, rows):
    tokens, width = x.shape
    part = wq.shape[1]
    heads = part // HEAD
    half = HEAD // 2
    depth, wide = wo.shape
    angle = np.arange(tokens, dtype=np.float32)[:, None] * np.float32(THETA) ** (-np.arange(half, dtype=np.float32) / np.float32(half))
    table = jnp.asarray(np.concatenate([np.cos(angle), np.sin(angle)], -1), jnp.float32)
    steps = tokens // rows
    any_ = pl.BlockSpec(memory_space=pl.ANY)
    now = lambda i: jnp.minimum(i, steps - 1)
    before = lambda i: jnp.maximum(i - 1, 0)
    normed = pltpu.VMEM((rows, width), jnp.bfloat16)
    dma = pltpu.SemaphoreType.DMA
    return pl.pallas_call(
        _project,
        grid=(steps + 1,),
        in_specs=[pl.BlockSpec((rows, width), lambda i: (now(i), 0)), pl.BlockSpec((1, width), lambda i: (0, 0)),
                  pl.BlockSpec((rows, HEAD), lambda i: (before(i), 0)), any_, any_, any_, any_],
        out_specs=[pl.BlockSpec((3 * heads, rows, HEAD), lambda i: (0, before(i), 0)), any_],
        out_shape=[jax.ShapeDtypeStruct((3 * heads, tokens, HEAD), jnp.bfloat16), jax.ShapeDtypeStruct((depth, wide // 2), jnp.bfloat16)],
        scratch_shapes=[normed, normed, pltpu.VMEM((width, 3 * part), jnp.bfloat16), dma((3,)), dma((PIECES,)), dma((PIECES,)), dma((2,))],
        compiler_params=pltpu.CompilerParams(dimension_semantics=("arbitrary",), vmem_limit_bytes=VMEM, collective_id=1, has_side_effects=True),
        cost_estimate=pl.CostEstimate(flops=6 * tokens * width * part, transcendentals=0, bytes_accessed=2 * width * (tokens + 3 * part)),
    )(x, gain[None], table, wq, wk, wv, wo)


def finish(qkv, wo, across, x, *, rows, keep, lags, ahead, tile, bq, bk):
    heads, tokens, d = qkv.shape[0] // 3, qkv.shape[1], qkv.shape[2]
    depth = heads * d
    wide = x.shape[1]
    quarter, half = wide // 4, wide // 8
    count = tokens // rows
    group, blocks = bq // rows, tokens // bq
    d2, d3, d4, d5, d6 = lags

    def kernel(qkv_ref, wo_ref, across_ref, x_ref, out_ref, seen4, wo4, big, sums, xs, acc_s, top_s, mix_s, gap_s,
               seen_sem, red_sem, own_sem, nbr_y, nbr_z, par_sem, dia_sem, wo_sem, local_sem, x_sem, send_sem):
        me = lax.axis_index("tp")
        y, z, c = me // 8, (me // 2) % 4, me % 2
        s = z // 2
        o = 1 - s
        inner = (z == 1) | (z == 2)
        at = lambda y, z, c: (y * 4 + z) * 2 + c
        partner, over = at(y, z, 1 - c), at(1 - y, z, c)
        peer = at(y, 3 - z, c)
        side = at(y, jnp.where(inner, 3 * s, 1 + s), c)
        block = y * 2 + c
        nblock = (1 - y) * 2 + c

        barrier = pltpu.get_barrier_semaphore()
        for who in (partner, over, side):
            pl.semaphore_signal(barrier, inc=1, device_id={"tp": who}, device_id_type=MESH)

        @pl.when(inner)
        def _():
            pl.semaphore_signal(barrier, inc=1, device_id={"tp": peer}, device_id_type=MESH)
            pl.semaphore_wait(barrier, 4)

        @pl.when(jnp.logical_not(inner))
        def _():
            pl.semaphore_wait(barrier, 3)

        def there(src, dst, kind, recv, who):
            pltpu.make_async_remote_copy(src_ref=src, dst_ref=dst, send_sem=send_sem.at[kind], recv_sem=recv, device_id={"tp": who},
                                         device_id_type=MESH).start()

        def arrived(dst, sem):
            pltpu.make_async_copy(dst, dst, sem).wait()

        def span(i):
            return pl.ds(pl.multiple_of(i * rows, rows), rows)

        def cols(q, h, a, b):
            return pl.ds(pl.multiple_of(q * quarter + h * half + a, 128), b - a)

        def blk(b):
            return pl.ds(pl.multiple_of(b * depth, 128), depth)

        def wo_part(src, side_block, h):
            return src.at[:, pl.ds(pl.multiple_of(side_block * quarter + h * half, 128), half)]

        def rows_of(b):
            return pl.ds(pl.multiple_of(b * depth, 128), depth)

        def group_span(b):
            return pl.ds(pl.multiple_of(b * bq, bq), bq)

        def see(b):
            attend_block(b, qkv_ref, seen4, block, top_s, mix_s, gap_s, bq, bk)
            got = seen4.at[group_span(b), blk(block)]
            there(got, got, 0, seen_sem.at[1, b], over)
            there(got, got, 1, seen_sem.at[0, b], partner)

        for h in range(2):
            there(wo_part(wo_ref, y * 2 + 1 - c, h), wo4.at[h, rows_of(block), :], 2, wo_sem.at[0, h], partner)
            there(wo_part(across_ref, 1 - c, h), wo4.at[h, rows_of(nblock), :], 3, wo_sem.at[1, h], partner)
            pltpu.make_async_copy(wo_part(wo_ref, y * 2 + c, h), wo4.at[h, rows_of(block), :], wo_sem.at[2, h]).start()
            pltpu.make_async_copy(wo_part(across_ref, c, h), wo4.at[h, rows_of(nblock), :], wo_sem.at[3, h]).start()

        pblock, dblock = y * 2 + 1 - c, (1 - y) * 2 + 1 - c

        def wo_wait():
            for h in range(2):
                arrived(wo4.at[h, rows_of(pblock), :], wo_sem.at[0, h])
                arrived(wo4.at[h, rows_of(dblock), :], wo_sem.at[1, h])
                arrived(wo4.at[h, rows_of(block), :], wo_sem.at[2, h])
                arrived(wo4.at[h, rows_of(nblock), :], wo_sem.at[3, h])

        gap_s[...] = lax.broadcasted_iota(jnp.int32, (bk, bq), 1) - lax.broadcasted_iota(jnp.int32, (bk, bq), 0)
        for b in range(ahead):
            see(b)

        def term(i, h, n):
            return jnp.dot(seen4[span(i), :], wo4[h, :, pl.ds(pl.multiple_of(n * tile, tile), tile)], preferred_element_type=jnp.float32)

        def tiles(body):
            def step(n, _):
                body(n, pl.ds(pl.multiple_of(n * tile, tile), tile))
            lax.fori_loop(0, half // tile, step, None)

        def seen_ready(i):
            @pl.when(lax.rem(i, group) == 0)
            def _():
                b = lax.div(i, group)
                arrived(seen4.at[group_span(b), blk(pblock)], seen_sem.at[0, b])
                arrived(seen4.at[group_span(b), blk(dblock)], seen_sem.at[2, b])

        def out_at(i, q, h, a=0, b=half):
            return out_ref.at[span(i), cols(q, h, a, b)]

        def x_copy(i):
            return pltpu.make_async_copy(x_ref.at[span(i), cols(block, s, 0, half)], xs.at[lax.rem(i, 2)], x_sem.at[lax.rem(i, 2)])

        def tick(t, _):
            on = lambda lag: (t >= lag) & (t - lag < count)

            b = lax.div(t, group)

            @pl.when((lax.rem(t, group) == 0) & (b < blocks))
            def _():
                got = seen4.at[group_span(b), blk(nblock)]
                arrived(got, seen_sem.at[1, b])
                there(got, got, 4, seen_sem.at[2, b], partner)

            @pl.when(t == min(d2, d3))
            def _():
                wo_wait()

            @pl.when(jnp.logical_not(inner))
            def _():
                @pl.when(on(d2))
                def _():
                    i = t - d2
                    seen_ready(i)
                    for k, h in enumerate((o, s)):
                        def put(n, at, h=h):
                            big[h, span(i), at] = term(i, h, n).astype(jnp.bfloat16)
                        tiles(put)
                        there(big.at[h, span(i), :], big.at[h, span(i), :], 5, red_sem.at[k, i], side)

                @pl.when(on(d6))
                def _():
                    i = t - d6
                    for h in (s, o):
                        arrived(out_at(i, block, h), own_sem.at[h, i])
                        if keep:
                            there(out_at(i, block, h, 0, keep), out_at(i, block, h, 0, keep), 6, nbr_y.at[h, i], over)
                        there(out_at(i, block, h), out_at(i, block, h), 7, par_sem.at[h, i], partner)

                @pl.when(on(d6 + 1))
                def _():
                    i = t - d6 - 1
                    for h in (s, o):
                        if keep < half:
                            arrived(out_at(i, nblock, h, keep, half), nbr_z.at[h, i])
                        if keep:
                            arrived(out_at(i, nblock, h, 0, keep), nbr_y.at[h, i])
                        there(out_at(i, nblock, h), out_at(i, nblock, h), 8, dia_sem.at[h, i], partner)

            @pl.when(inner)
            def _():
                @pl.when(on(d3))
                def _():
                    i = t - d3
                    seen_ready(i)
                    arrived(big.at[o, span(i), :], red_sem.at[0, i])

                    def add(n, at):
                        sums[o, span(i), at] = (term(i, o, n) + big[o, span(i), at].astype(jnp.float32)).astype(jnp.bfloat16)
                    tiles(add)
                    there(sums.at[o, span(i), :], sums.at[o, span(i), :], 9, red_sem.at[2, i], peer)
                    x_copy(i).start()

                @pl.when(on(d4))
                def _():
                    i = t - d4
                    slot = lax.rem(i, 2)
                    x_copy(i).wait()
                    arrived(big.at[s, span(i), :], red_sem.at[1, i])

                    def before(n, at):
                        acc_s[:, at] = term(i, s, n) + big[s, span(i), at].astype(jnp.float32) + xs[slot, :, at].astype(jnp.float32)
                    tiles(before)
                    arrived(sums.at[s, span(i), :], red_sem.at[2, i])

                    def add(n, at):
                        big[s, span(i), at] = (acc_s[:, at] + sums[s, span(i), at].astype(jnp.float32)).astype(jnp.bfloat16)
                    tiles(add)
                    done = big.at[s, span(i), :]
                    there(done, out_at(i, block, s), 10, own_sem.at[s, i], peer)
                    there(done, out_at(i, block, s), 11, own_sem.at[s, i], side)
                    if keep < half:
                        there(big.at[s, span(i), pl.ds(keep, half - keep)], out_at(i, block, s, keep, half), 12, nbr_z.at[s, i], over)
                    if keep:
                        there(big.at[s, span(i), pl.ds(0, keep)], out_at(i, block, s, 0, keep), 6, nbr_y.at[s, i], over)
                    there(done, out_at(i, block, s), 7, par_sem.at[s, i], partner)
                    pltpu.make_async_copy(done, out_at(i, block, s), local_sem.at[1]).start()

                @pl.when(on(d5))
                def _():
                    i = t - d5
                    arrived(out_at(i, block, o), own_sem.at[o, i])
                    there(out_at(i, block, o), out_at(i, block, o), 13, own_sem.at[o, i], side)
                    if keep:
                        there(out_at(i, block, o, 0, keep), out_at(i, block, o, 0, keep), 6, nbr_y.at[o, i], over)
                    there(out_at(i, block, o), out_at(i, block, o), 7, par_sem.at[o, i], partner)
                    if keep < half:
                        far = out_at(i, nblock, s, keep, half)
                        arrived(far, nbr_z.at[s, i])
                        there(far, far, 14, nbr_z.at[s, i], peer)
                        there(far, far, 15, nbr_z.at[s, i], side)
                    if keep:
                        arrived(out_at(i, nblock, s, 0, keep), nbr_y.at[s, i])
                    there(out_at(i, nblock, s), out_at(i, nblock, s), 8, dia_sem.at[s, i], partner)

                @pl.when(on(d5 + 1))
                def _():
                    i = t - d5 - 1
                    if keep < half:
                        far = out_at(i, nblock, o, keep, half)
                        arrived(far, nbr_z.at[o, i])
                        there(far, far, 16, nbr_z.at[o, i], side)
                    if keep:
                        arrived(out_at(i, nblock, o, 0, keep), nbr_y.at[o, i])
                    there(out_at(i, nblock, o), out_at(i, nblock, o), 8, dia_sem.at[o, i], partner)

            @pl.when((lax.rem(t, group) == 0) & (b + ahead < blocks))
            def _():
                see(b + ahead)

        lax.fori_loop(0, count + max(d5, d6) + 1, tick, None)

        def last(i, _):
            for h in range(2):
                arrived(out_at(i, pblock, h), par_sem.at[h, i])
                arrived(out_at(i, dblock, h), dia_sem.at[h, i])
        lax.fori_loop(0, count, last, None)

        def sent(kind, ref):
            pltpu.make_async_copy(ref, ref, send_sem.at[kind]).wait()

        whole = seen4.at[:, pl.ds(0, depth)]
        sent(0, whole)
        sent(1, whole)
        sent(2, wo4.at[:, pl.ds(0, depth), :])
        sent(3, wo4.at[:, pl.ds(0, depth), :])
        sent(4, whole)
        full = lambda n, a, b: out_ref.at[:, pl.ds(0, n * (b - a))]
        if keep:
            sent(6, full(2, 0, keep))
        sent(7, full(2, 0, half))
        sent(8, full(2, 0, half))

        @pl.when(jnp.logical_not(inner))
        def _():
            sent(5, big)

        @pl.when(inner)
        def _():
            sent(9, full(1, 0, half))
            sent(10, full(1, 0, half))
            sent(11, full(1, 0, half))
            sent(13, full(1, 0, half))
            if keep < half:
                for kind in (12, 14, 15, 16):
                    sent(kind, full(1, keep, half))
            pltpu.make_async_copy(big.at[0], big.at[0], local_sem.at[1]).wait()

    any_ = pl.BlockSpec(memory_space=pl.ANY)
    dma = pltpu.SemaphoreType.DMA
    return pl.pallas_call(
        kernel,
        out_shape=jax.ShapeDtypeStruct((tokens, wide), jnp.bfloat16),
        in_specs=[pl.BlockSpec(memory_space=pltpu.VMEM)] + [any_] * 3,
        out_specs=any_,
        scratch_shapes=[
            pltpu.VMEM((tokens, 4 * depth), jnp.bfloat16),
            pltpu.VMEM((2, 4 * depth, half), jnp.bfloat16),
            pltpu.VMEM((2, tokens, half), jnp.bfloat16),
            pltpu.VMEM((2, tokens, half), jnp.bfloat16),
            pltpu.VMEM((2, rows, half), jnp.bfloat16),
            pltpu.VMEM((rows, half), jnp.float32),
            pltpu.VMEM((heads, bq), jnp.float32), pltpu.VMEM((heads, d + 8, bq), jnp.float32), pltpu.VMEM((bk, bq), jnp.int32),
            dma((3, blocks)), dma((3, count)), dma((2, count)), dma((2, count)), dma((2, count)), dma((2, count)), dma((2, count)),
            dma((4, 2)), dma((2,)), dma((2,)), dma((17,)),
        ],
        compiler_params=pltpu.CompilerParams(collective_id=0, has_side_effects=True, vmem_limit_bytes=56 * 2**20),
        cost_estimate=pl.CostEstimate(flops=2 * tokens * 4 * depth * quarter, transcendentals=0, bytes_accessed=4 * tokens * wide),
    )(qkv, wo, across, x)


LAGS = (2, 3, 4, 6, 8)
ROWS = 64
KEEP = 896


def solution(mesh):
    def step(x, gain, wq, wk, wv, wo):
        qkv, across = project(x, gain, wq, wk, wv, wo, 256)
        return finish(qkv, wo, across, x, rows=ROWS, keep=KEEP, lags=LAGS, ahead=1, tile=256, bq=128, bk=256)

    tokens, columns = P("dp", None), P(None, "tp")
    return jax.shard_map(
        step,
        mesh=mesh,
        in_specs=(tokens, P(None), columns, columns, columns, P("tp", None)),
        out_specs=tokens,
        check_vma=False,
    )
```

```python
import jax
import jax.numpy as jnp
import numpy as np
from jax import lax
from jax.experimental import pallas as pl
from jax.experimental.pallas import tpu as pltpu
from jax.sharding import PartitionSpec as P

HEAD = 128
THETA = 10000
NEG = -1e30
HIDDEN = 2 * NEG
LOG2E = 1.4426950408889634
MESH = pl.DeviceIdType.MESH
VMEM = 56 * 2**20


def _dot(a, b, ca, cb):
    return lax.dot_general(a, b, (((ca,), (cb,)), ((), ())), preferred_element_type=jnp.float32)


def attend_block(b, qkv_ref, o_ref, place, top_s, mix_s, gap_s, bq, bk):
    heads, d = qkv_ref.shape[0] // 3, qkv_ref.shape[2]
    low = qkv_ref.dtype
    e = d**-0.5 * LOG2E
    queries = pl.ds(pl.multiple_of(b * bq, bq), bq)
    top_s[...] = jnp.full(top_s.shape, NEG, jnp.float32)
    mix_s[...] = jnp.zeros(mix_s.shape, jnp.float32)

    def block(j, masked):
        size = bq if masked else bk
        here = pl.ds(pl.multiple_of(j * size, size), size)
        ones = jnp.ones((8, size), low)
        scores = [_dot(qkv_ref[heads + i, here, :], qkv_ref[i, queries, :], 1, 1) for i in range(heads)]
        ok = gap_s[...] >= (j - b) * bq if masked else None
        weights, keeps = [], []
        for i, s in enumerate(scores):
            if masked:
                s = jnp.where(ok, s, HIDDEN)
            old = top_s[i : i + 1, :]
            top = jnp.maximum(old, s.max(axis=0, keepdims=True))
            top_s[i : i + 1, :] = top
            weights.append(jnp.exp2((s - top) * e).astype(low))
            keeps.append(jnp.exp2((old - top) * e))
        for i, (p, keep) in enumerate(zip(weights, keeps)):
            values = jnp.concatenate([qkv_ref[2 * heads + i, here, :].T, ones], axis=0)
            mix_s[i] = mix_s[i] * keep + _dot(values, p, 1, 0)

    whole = lax.div(b * bq, bk)
    lax.fori_loop(0, whole, lambda j, _: block(j, False), None)
    lax.fori_loop(whole * (bk // bq), b + 1, lambda j, _: block(j, True), None)
    for i in range(heads):
        got = (mix_s[i, :d, :] * (1 / mix_s[i, d : d + 1, :])).T.astype(o_ref.dtype)
        o_ref[queries, pl.ds(pl.multiple_of((place * heads + i) * d, d), d)] = got


PIECES = 16


def norm_rows(x_ref, to, gain_ref, at, count):
    width = x_ref.shape[1]
    for r in range(0, count, 16):
        here = pl.ds(at + r, 16)
        total = jnp.zeros((16, HEAD), jnp.float32)
        for c in range(0, width, HEAD):
            wide = x_ref[here, c : c + HEAD].astype(jnp.float32)
            total += wide * wide
        scale = lax.rsqrt(total.sum(-1, keepdims=True) * (1 / width) + 1e-6)
        for c in range(0, width, HEAD):
            wide = x_ref[here, c : c + HEAD].astype(jnp.float32)
            to[here, c : c + HEAD] = (wide * scale * gain_ref[:, c : c + HEAD].astype(jnp.float32)).astype(jnp.bfloat16)


def two_heads(a_ref, w_s, n, table):
    tile = 2 * HEAD
    got = _dot(a_ref[...], w_s[:, pl.ds(pl.multiple_of(n * tile, tile), tile)], 1, 0).astype(jnp.bfloat16)
    swapped = pltpu.roll(table, HEAD // 2, 1)
    first = lax.broadcasted_iota(jnp.int32, table.shape, 1) < HEAD // 2
    turn = n < 2 * w_s.shape[1] // 3 // tile
    cos = jnp.where(turn, jnp.where(first, table, swapped), 1.0)
    sin = jnp.where(turn, jnp.where(first, -swapped, table), 0.0)
    parts = [got[:, h * HEAD : (h + 1) * HEAD].astype(jnp.float32) for h in range(2)]
    return [(t * cos + pltpu.roll(t, HEAD // 2, 1) * sin).astype(jnp.bfloat16) for t in parts]


def _project(x_ref, gain_ref, table_ref, wq_ref, wk_ref, wv_ref, wo_ref, out_ref, across_ref, even_s, odd_s, w_s, w_sem, y_sem, x_sem, send_sem):
    i, last = pl.program_id(0), pl.num_programs(0) - 1
    me, dp = lax.axis_index("tp"), lax.axis_index("dp")
    y = me // 8
    over = lax.rem(me + 8, 16)
    rows, width = even_s.shape
    part = wq_ref.shape[1]
    tile = 2 * HEAD
    tiles = 3 * part // tile
    lot = -(-rows // tiles // 16) * 16
    copies = [pltpu.make_async_copy(src, w_s.at[:, pl.ds(n * part, part)], w_sem.at[n]) for n, src in enumerate((wq_ref, wk_ref, wv_ref))]
    depth, side = across_ref.shape
    few = depth // 2 // PIECES

    def piece(ref, d, n, at):
        return ref.at[pl.ds(pl.multiple_of(d * (depth // 2) + n * few, few), few), pl.ds(pl.multiple_of(at, 128), side)]

    @pl.when(i == 0)
    def _():
        for copy in copies:
            copy.start()
        barrier = pltpu.get_barrier_semaphore()
        pl.semaphore_signal(barrier, inc=1, device_id={"tp": over}, device_id_type=MESH)
        pl.semaphore_signal(barrier, inc=1, device_id={"dp": 1 - dp}, device_id_type=MESH)
        pl.semaphore_wait(barrier, 2)

        def send(n, _):
            pltpu.make_async_remote_copy(src_ref=piece(wo_ref, dp, n, (1 - y) * side), dst_ref=piece(across_ref, dp, n, 0), send_sem=send_sem.at[0],
                                         recv_sem=y_sem.at[n], device_id={"tp": over}, device_id_type=MESH).start()
        lax.fori_loop(0, PIECES, send, None)

    def arrived(ref, sem):
        pltpu.make_async_copy(ref, ref, sem).wait()

    def forward(n):
        ref = piece(across_ref, dp, n, 0)
        arrived(ref, y_sem.at[n])
        pltpu.make_async_remote_copy(src_ref=ref, dst_ref=ref, send_sem=send_sem.at[1], recv_sem=x_sem.at[n], device_id={"dp": 1 - dp},
                                     device_id_type=MESH).start()

    def norm(to, n):
        norm_rows(x_ref, to, gain_ref, pl.multiple_of(jnp.minimum(n * lot, rows - lot), 16), lot)

    def product(of, n):
        for h, t in enumerate(two_heads(of, w_s, n, table_ref[...])):
            out_ref[2 * n + h] = t

    def both(of, to):
        def step(n, _):
            @pl.when((i == 1) & (lax.rem(n, part // tile) == 0))
            def _():
                arrived(w_s.at[:, pl.ds(0, part)], w_sem.at[lax.div(n, part // tile)])

            product(of, n)
            norm(to, n)
        lax.fori_loop(0, tiles, step, None)

    @pl.when(i == 0)
    def _():
        lax.fori_loop(0, tiles, lambda n, _: norm(even_s, n), None)

    @pl.when(i > 0)
    def _():
        def some(n, _):
            forward(n)
        lax.fori_loop(lax.div((i - 1) * PIECES, last), lax.div(i * PIECES, last), some, None)

    odd = lax.rem(i, 2) == 1

    @pl.when(odd)
    def _():
        both(even_s, odd_s)

    @pl.when((i > 0) & jnp.logical_not(odd))
    def _():
        both(odd_s, even_s)

    @pl.when(i == last)
    def _():
        def end(n, _):
            arrived(piece(across_ref, 1 - dp, n, 0), x_sem.at[n])
        lax.fori_loop(0, PIECES, end, None)
        half = across_ref.at[pl.ds(0, depth // 2), :]
        arrived(half, send_sem.at[0])
        arrived(half, send_sem.at[1])


def turns(tokens):
    half = HEAD // 2
    angle = np.arange(tokens, dtype=np.float32)[:, None] * np.float32(THETA) ** (-np.arange(half, dtype=np.float32) / np.float32(half))
    return np.concatenate([np.cos(angle), np.sin(angle)], -1).astype(np.float32)


def project(x, gain, table, wq, wk, wv, wo, rows, tokens):
    width = x.shape[1]
    part = wq.shape[1]
    heads = part // HEAD
    depth, wide = wo.shape
    steps = tokens // rows
    any_ = pl.BlockSpec(memory_space=pl.ANY)
    now = lambda i: jnp.minimum(i, steps - 1)
    before = lambda i: jnp.maximum(i - 1, 0)
    normed = pltpu.VMEM((rows, width), jnp.bfloat16)
    dma = pltpu.SemaphoreType.DMA
    return pl.pallas_call(
        _project,
        grid=(steps + 1,),
        in_specs=[pl.BlockSpec((rows, width), lambda i: (now(i), 0)), pl.BlockSpec((1, width), lambda i: (0, 0)),
                  pl.BlockSpec((rows, HEAD), lambda i: (before(i), 0)), any_, any_, any_, any_],
        out_specs=[pl.BlockSpec((3 * heads, rows, HEAD), lambda i: (0, before(i), 0)), any_],
        out_shape=[jax.ShapeDtypeStruct((3 * heads, tokens, HEAD), jnp.bfloat16), jax.ShapeDtypeStruct((depth, wide // 2), jnp.bfloat16)],
        scratch_shapes=[normed, normed, pltpu.VMEM((width, 3 * part), jnp.bfloat16), dma((3,)), dma((PIECES,)), dma((PIECES,)), dma((2,))],
        compiler_params=pltpu.CompilerParams(dimension_semantics=("arbitrary",), vmem_limit_bytes=VMEM, collective_id=1, has_side_effects=True),
        cost_estimate=pl.CostEstimate(flops=6 * tokens * width * part, transcendentals=0, bytes_accessed=2 * width * (tokens + 3 * part)),
    )(x, gain[None], table, wq, wk, wv, wo)


def finish(qkv, gain, table, wq, wk, wv, wo, across, x, *, rows, keep, lags, ahead, pace, apart, tile, bq, bk):
    heads, some, d = qkv.shape[0] // 3, qkv.shape[1], qkv.shape[2]
    tokens = x.shape[0]
    depth = heads * d
    wide = x.shape[1]
    quarter, half = wide // 4, wide // 8
    count = tokens // rows
    group, blocks = bq // rows, tokens // bq
    given = some // bq
    d2, d3, d4, d5, d6 = lags

    def kernel(table_ref, gain_ref, qkv_ref, wq_ref, wk_ref, wv_ref, wo_ref, across_ref, x_ref, out_ref, qkv_s, w_s, a_s, seen4, wo4, big, sums, xs,
               acc_s, top_s, mix_s, gap_s,
               seen_sem, red_sem, own_sem, nbr_y, nbr_z, par_sem, dia_sem, wo_sem, local_sem, x_sem, in_sem, send_sem):
        me = lax.axis_index("tp")
        y, z, c = me // 8, (me // 2) % 4, me % 2
        s = z // 2
        o = 1 - s
        inner = (z == 1) | (z == 2)
        at = lambda y, z, c: (y * 4 + z) * 2 + c
        partner, over = at(y, z, 1 - c), at(1 - y, z, c)
        peer = at(y, 3 - z, c)
        side = at(y, jnp.where(inner, 3 * s, 1 + s), c)
        block = y * 2 + c
        nblock = (1 - y) * 2 + c

        barrier = pltpu.get_barrier_semaphore()
        for who in (partner, over, side):
            pl.semaphore_signal(barrier, inc=1, device_id={"tp": who}, device_id_type=MESH)

        @pl.when(inner)
        def _():
            pl.semaphore_signal(barrier, inc=1, device_id={"tp": peer}, device_id_type=MESH)
            pl.semaphore_wait(barrier, 4)

        @pl.when(jnp.logical_not(inner))
        def _():
            pl.semaphore_wait(barrier, 3)

        def there(src, dst, kind, recv, who):
            pltpu.make_async_remote_copy(src_ref=src, dst_ref=dst, send_sem=send_sem.at[kind], recv_sem=recv, device_id={"tp": who},
                                         device_id_type=MESH).start()

        def arrived(dst, sem):
            pltpu.make_async_copy(dst, dst, sem).wait()

        def span(i):
            return pl.ds(pl.multiple_of(i * rows, rows), rows)

        def cols(q, h, a, b):
            return pl.ds(pl.multiple_of(q * quarter + h * half + a, 128), b - a)

        def blk(b):
            return pl.ds(pl.multiple_of(b * depth, 128), depth)

        def wo_part(src, side_block, h):
            return src.at[:, pl.ds(pl.multiple_of(side_block * quarter + h * half, 128), half)]

        def rows_of(b):
            return pl.ds(pl.multiple_of(b * depth, 128), depth)

        def group_span(b):
            return pl.ds(pl.multiple_of(b * bq, bq), bq)

        def see(b):
            attend_block(b, qkv_s, seen4, block, top_s, mix_s, gap_s, bq, bk)
            got = seen4.at[group_span(b), blk(block)]
            there(got, got, 0, seen_sem.at[1, b], over)
            there(got, got, 1, seen_sem.at[0, b], partner)

        for h in range(2):
            there(wo_part(wo_ref, y * 2 + 1 - c, h), wo4.at[h, rows_of(block), :], 2, wo_sem.at[0, h], partner)
            there(wo_part(across_ref, 1 - c, h), wo4.at[h, rows_of(nblock), :], 3, wo_sem.at[1, h], partner)
            pltpu.make_async_copy(wo_part(wo_ref, y * 2 + c, h), wo4.at[h, rows_of(block), :], wo_sem.at[2, h]).start()
            pltpu.make_async_copy(wo_part(across_ref, c, h), wo4.at[h, rows_of(nblock), :], wo_sem.at[3, h]).start()

        pblock, dblock = y * 2 + 1 - c, (1 - y) * 2 + 1 - c

        def wo_wait():
            for h in range(2):
                arrived(wo4.at[h, rows_of(pblock), :], wo_sem.at[0, h])
                arrived(wo4.at[h, rows_of(dblock), :], wo_sem.at[1, h])
                arrived(wo4.at[h, rows_of(block), :], wo_sem.at[2, h])
                arrived(wo4.at[h, rows_of(nblock), :], wo_sem.at[3, h])

        known = pltpu.make_async_copy(qkv_ref, qkv_s.at[:, pl.ds(0, some), :], local_sem.at[0])
        known.start()
        width = w_s.shape[1] // 3
        loads = [pltpu.make_async_copy(src, w_s.at[:, pl.ds(n * width, width)], in_sem.at[n]) for n, src in enumerate((wq_ref, wk_ref, wv_ref))]

        def next_x(n):
            return pltpu.make_async_copy(x_ref.at[group_span(given + n), :], a_s, in_sem.at[3])

        next_x(0).start()
        for load in loads:
            load.start()

        def project_block(n, phase):
            here = group_span(given + n)

            @pl.when(phase == 0)
            def _():
                next_x(n).wait()
                lax.fori_loop(0, bq // 16, lambda r, _: norm_rows(a_s, a_s, gain_ref, pl.multiple_of(r * 16, 16), 16), None)

            each = 3 * heads // 2 // (apart - 1)

            @pl.when(phase > 0)
            def _():
                def pair(m, _):
                    for h, got in enumerate(two_heads(a_s, w_s, m, table_ref[group_span(n), :])):
                        qkv_s[2 * m + h, here, :] = got
                lax.fori_loop((phase - 1) * each, phase * each, pair, None)

            @pl.when((phase == apart - 1) & (n + 1 < blocks - given))
            def _():
                next_x(n + 1).start()

        known.wait()
        gap_s[...] = lax.broadcasted_iota(jnp.int32, (bq, bq), 1) - lax.broadcasted_iota(jnp.int32, (bq, bq), 0)
        for b in range(ahead):
            see(b)

        def term(i, h, n):
            return jnp.dot(seen4[span(i), :], wo4[h, :, pl.ds(pl.multiple_of(n * tile, tile), tile)], preferred_element_type=jnp.float32)

        def tiles(body):
            def step(n, _):
                body(n, pl.ds(pl.multiple_of(n * tile, tile), tile))
            lax.fori_loop(0, half // tile, step, None)

        def seen_ready(i):
            @pl.when(lax.rem(i, group) == 0)
            def _():
                b = lax.div(i, group)
                arrived(seen4.at[group_span(b), blk(pblock)], seen_sem.at[0, b])
                arrived(seen4.at[group_span(b), blk(dblock)], seen_sem.at[2, b])

        def out_at(i, q, h, a=0, b=half):
            return out_ref.at[span(i), cols(q, h, a, b)]

        def x_copy(i):
            return pltpu.make_async_copy(x_ref.at[span(i), cols(block, s, 0, half)], xs.at[lax.rem(i, 2)], x_sem.at[lax.rem(i, 2)])

        def tick(t, _):
            on = lambda lag: (t >= lag) & (t - lag < count)

            b = lax.div(t, group)

            @pl.when((lax.rem(t, group) == 0) & (b < blocks))
            def _():
                got = seen4.at[group_span(b), blk(nblock)]
                arrived(got, seen_sem.at[1, b])
                there(got, got, 4, seen_sem.at[2, b], partner)

            @pl.when(t == min(d2, d3))
            def _():
                wo_wait()

            @pl.when(jnp.logical_not(inner))
            def _():
                @pl.when(on(d2))
                def _():
                    i = t - d2
                    seen_ready(i)
                    for k, h in enumerate((o, s)):
                        def put(n, at, h=h):
                            big[h, span(i), at] = term(i, h, n).astype(jnp.bfloat16)
                        tiles(put)
                        there(big.at[h, span(i), :], big.at[h, span(i), :], 5, red_sem.at[k, i], side)

                @pl.when(on(d6))
                def _():
                    i = t - d6
                    for h in (s, o):
                        arrived(out_at(i, block, h), own_sem.at[h, i])
                        if keep:
                            there(out_at(i, block, h, 0, keep), out_at(i, block, h, 0, keep), 6, nbr_y.at[h, i], over)
                        there(out_at(i, block, h), out_at(i, block, h), 7, par_sem.at[h, i], partner)

                @pl.when(on(d6 + 1))
                def _():
                    i = t - d6 - 1
                    for h in (s, o):
                        if keep < half:
                            arrived(out_at(i, nblock, h, keep, half), nbr_z.at[h, i])
                        if keep:
                            arrived(out_at(i, nblock, h, 0, keep), nbr_y.at[h, i])
                        there(out_at(i, nblock, h), out_at(i, nblock, h), 8, dia_sem.at[h, i], partner)

            @pl.when(inner)
            def _():
                @pl.when(on(d3))
                def _():
                    i = t - d3
                    seen_ready(i)
                    arrived(big.at[o, span(i), :], red_sem.at[0, i])

                    def add(n, at):
                        big[o, span(i), at] = (term(i, o, n) + big[o, span(i), at].astype(jnp.float32)).astype(jnp.bfloat16)
                    tiles(add)
                    there(big.at[o, span(i), :], sums.at[span(i), :], 9, red_sem.at[2, i], peer)
                    x_copy(i).start()

                @pl.when(on(d4))
                def _():
                    i = t - d4
                    slot = lax.rem(i, 2)
                    x_copy(i).wait()
                    arrived(big.at[s, span(i), :], red_sem.at[1, i])

                    def before(n, at):
                        acc_s[:, at] = term(i, s, n) + big[s, span(i), at].astype(jnp.float32) + xs[slot, :, at].astype(jnp.float32)
                    tiles(before)
                    arrived(sums.at[span(i), :], red_sem.at[2, i])

                    def add(n, at):
                        big[s, span(i), at] = (acc_s[:, at] + sums[span(i), at].astype(jnp.float32)).astype(jnp.bfloat16)
                    tiles(add)
                    done = big.at[s, span(i), :]
                    there(done, out_at(i, block, s), 10, own_sem.at[s, i], peer)
                    there(done, out_at(i, block, s), 11, own_sem.at[s, i], side)
                    if keep < half:
                        there(big.at[s, span(i), pl.ds(keep, half - keep)], out_at(i, block, s, keep, half), 12, nbr_z.at[s, i], over)
                    if keep:
                        there(big.at[s, span(i), pl.ds(0, keep)], out_at(i, block, s, 0, keep), 6, nbr_y.at[s, i], over)
                    there(done, out_at(i, block, s), 7, par_sem.at[s, i], partner)
                    pltpu.make_async_copy(done, out_at(i, block, s), local_sem.at[1]).start()

                @pl.when(on(d5))
                def _():
                    i = t - d5
                    arrived(out_at(i, block, o), own_sem.at[o, i])
                    there(out_at(i, block, o), out_at(i, block, o), 13, own_sem.at[o, i], side)
                    if keep:
                        there(out_at(i, block, o, 0, keep), out_at(i, block, o, 0, keep), 6, nbr_y.at[o, i], over)
                    there(out_at(i, block, o), out_at(i, block, o), 7, par_sem.at[o, i], partner)
                    if keep < half:
                        far = out_at(i, nblock, s, keep, half)
                        arrived(far, nbr_z.at[s, i])
                        there(far, far, 14, nbr_z.at[s, i], peer)
                        there(far, far, 15, nbr_z.at[s, i], side)
                    if keep:
                        arrived(out_at(i, nblock, s, 0, keep), nbr_y.at[s, i])
                    there(out_at(i, nblock, s), out_at(i, nblock, s), 8, dia_sem.at[s, i], partner)

                @pl.when(on(d5 + 1))
                def _():
                    i = t - d5 - 1
                    if keep < half:
                        far = out_at(i, nblock, o, keep, half)
                        arrived(far, nbr_z.at[o, i])
                        there(far, far, 16, nbr_z.at[o, i], side)
                    if keep:
                        arrived(out_at(i, nblock, o, 0, keep), nbr_y.at[o, i])
                    there(out_at(i, nblock, o), out_at(i, nblock, o), 8, dia_sem.at[o, i], partner)

            @pl.when((lax.rem(t, pace) == 0) & (lax.div(t, pace) + ahead < blocks))
            def _():
                see(lax.div(t, pace) + ahead)

            @pl.when(t == 1)
            def _():
                for load in loads:
                    load.wait()

            n = lax.div(t, apart)

            @pl.when(n < blocks - given)
            def _():
                project_block(n, lax.rem(t, apart))

        lax.fori_loop(0, count + max(d5, d6) + 1, tick, None)

        def last(i, _):
            for h in range(2):
                arrived(out_at(i, pblock, h), par_sem.at[h, i])
                arrived(out_at(i, dblock, h), dia_sem.at[h, i])
        lax.fori_loop(0, count, last, None)

        def sent(kind, ref):
            pltpu.make_async_copy(ref, ref, send_sem.at[kind]).wait()

        whole = seen4.at[:, pl.ds(0, depth)]
        sent(0, whole)
        sent(1, whole)
        sent(2, wo4.at[:, pl.ds(0, depth), :])
        sent(3, wo4.at[:, pl.ds(0, depth), :])
        sent(4, whole)
        full = lambda n, a, b: out_ref.at[:, pl.ds(0, n * (b - a))]
        if keep:
            sent(6, full(2, 0, keep))
        sent(7, full(2, 0, half))
        sent(8, full(2, 0, half))

        @pl.when(jnp.logical_not(inner))
        def _():
            sent(5, big)

        @pl.when(inner)
        def _():
            sent(9, full(1, 0, half))
            sent(10, full(1, 0, half))
            sent(11, full(1, 0, half))
            sent(13, full(1, 0, half))
            if keep < half:
                for kind in (12, 14, 15, 16):
                    sent(kind, full(1, keep, half))
            pltpu.make_async_copy(big.at[0], big.at[0], local_sem.at[1]).wait()

    any_ = pl.BlockSpec(memory_space=pl.ANY)
    dma = pltpu.SemaphoreType.DMA
    return pl.pallas_call(
        kernel,
        out_shape=jax.ShapeDtypeStruct((tokens, wide), jnp.bfloat16),
        in_specs=[pl.BlockSpec(memory_space=pltpu.VMEM)] * 2 + [any_] * 7,
        out_specs=any_,
        scratch_shapes=[
            pltpu.VMEM((3 * heads, tokens, d), jnp.bfloat16),
            pltpu.VMEM((wide, 3 * depth), jnp.bfloat16),
            pltpu.VMEM((bq, wide), jnp.bfloat16),
            pltpu.VMEM((tokens, 4 * depth), jnp.bfloat16),
            pltpu.VMEM((2, 4 * depth, half), jnp.bfloat16),
            pltpu.VMEM((2, tokens, half), jnp.bfloat16),
            pltpu.VMEM((tokens, half), jnp.bfloat16),
            pltpu.VMEM((2, rows, half), jnp.bfloat16),
            pltpu.VMEM((rows, half), jnp.float32),
            pltpu.VMEM((heads, bq), jnp.float32), pltpu.VMEM((heads, d + 8, bq), jnp.float32), pltpu.VMEM((bq, bq), jnp.int32),
            dma((3, blocks)), dma((3, count)), dma((2, count)), dma((2, count)), dma((2, count)), dma((2, count)), dma((2, count)),
            dma((4, 2)), dma((2,)), dma((2,)), dma((4,)), dma((17,)),
        ],
        compiler_params=pltpu.CompilerParams(collective_id=0, has_side_effects=True, vmem_limit_bytes=67043328),
        cost_estimate=pl.CostEstimate(flops=2 * tokens * 4 * depth * quarter, transcendentals=0, bytes_accessed=4 * tokens * wide),
    )(table, gain[None], qkv, wq, wk, wv, wo, across, x)


LAGS = (1, 2, 3, 4, 5)
FIRST = 1280
ROWS = 64
KEEP = 896


def solution(mesh):
    def step(x, gain, wq, wk, wv, wo):
        table = turns(x.shape[0])
        qkv, across = project(x, gain, jnp.asarray(table[:FIRST]), wq, wk, wv, wo, 256, FIRST)
        return finish(qkv, gain, jnp.asarray(table[FIRST:]), wq, wk, wv, wo, across, x, rows=ROWS, keep=KEEP, lags=LAGS, ahead=1, pace=2, apart=4,
                      tile=256, bq=128, bk=256)

    tokens, columns = P("dp", None), P(None, "tp")
    return jax.shard_map(
        step,
        mesh=mesh,
        in_specs=(tokens, P(None), columns, columns, columns, P("tp", None)),
        out_specs=tokens,
        check_vma=False,
    )
```
